256 devices in a mesh: grid: 8 (over z), orb: 16 (over y, x_hi, core), pts: 2 (over x_lo).
Axes of the slice: x: 4 (x_hi: 2, x_lo: 2; x = x_hi * 2 + x_lo), y: 4, z: 8, core: 2. Of those that a mesh axis runs over, the one named last changes fastest.
Arguments:
- orbitals: bfloat16 [2048, 2048], P('grid', 'orb'), may hold values from -6 to 6
- points: int32 [8192], replicated, may hold values from 0 to 2047
- fitting: bfloat16 [2048, 8192], P('grid', ('orb', 'pts')), may hold values from -0.0625 to 0.0625
- screened: bfloat16 [8192, 8192], P(('orb', 'pts'), 'grid'), may hold values from -0.0014648438 to 0.0014648438
Outputs:
- exchange_orbitals: float32 [2048, 2048], P(('orb', 'pts'), 'grid')
- exchange_matrix: float32 [2048, 2048], P(('orb', 'pts'), 'grid')
The draws below stay inside these ranges and needn't reach their ends.
Inputs may be any that keep to these rules, and one draw needn't show every extreme that they name: Grid rows of the window; two points may name the same row.
All inputs are finite; a program needn't handle non-finite values.
Results may differ from the reference program's by a relative error of at most 0.005.
Values may be sent and summed in bfloat16 or wider, within the bound.
No kernel may reach another device: no remote copies, remote signals or barrier semaphores. Data moves between devices by JAX's collectives and lax.ppermute only.
A program may use at most 128 MiB of HBM per device.

```python
import math
import jax
import jax.numpy as jnp

NO = 2048
NP = 8192
NR = 2048


def place_ends(values, rng, low, largest):
    longest = values.shape.index(max(values.shape))
    spots = []
    for shift in (0, 1):
        where = [jax.random.randint(jax.random.fold_in(rng, axis), (), 0, length) for axis, length in enumerate(values.shape)]
        where[longest] = (where[longest] + shift) % values.shape[longest]
        spots.append(tuple(where))
    return values.at[spots[0]].set(low).at[spots[1]].set(largest)


def levels(rng, shape, split, low, high):
    def one(axis_at, blocks):
        heights = jax.random.uniform(jax.random.fold_in(jax.random.fold_in(rng, 6), axis_at), (blocks,), jnp.float32, low / len(split), high / len(split))
        return jnp.repeat(jnp.exp(heights), shape[axis_at] // blocks).reshape((-1,) + (1,) * (len(shape) - axis_at - 1))

    factor_of = one(*split[0])
    for cut in split[1:]:
        factor_of = factor_of * one(*cut)
    return factor_of


def scatter_about(rng, shape, scale, limit, cuts=(), held_as=jnp.bfloat16):
    array = jax.random.normal(rng, shape, jnp.float32) * scale
    if len(cuts) > 0:
        array = levels(rng, shape, cuts, -0.22, 0.18) * array
    return jnp.clip(array, min=-limit, max=limit).astype(held_as)


def setup_inputs(seed: int = 0) -> dict:
    streams_of = jax.random.split(jax.random.key(seed), 5)
    orbitals = scatter_about(streams_of[0], (NR, NO), 1.0, 6.0, ((0, 8), (1, 16)))
    points = place_ends(jax.random.randint(streams_of[1], (NP,), 0, NR), jax.random.fold_in(streams_of[1], 1), 0, NR - 1).astype(jnp.int32)
    fitting = scatter_about(streams_of[2], (NR, NP), NP ** -0.5, 0.0625, ((0, 8), (1, 32)))
    screened = scatter_about(streams_of[3], (NP, NP), (NP * NO) ** -0.5, 0.0014648438, ((0, 32), (1, 8)))
    return dict(orbitals=orbitals, points=points, fitting=fitting, screened=screened)


def reference(orbitals, points, fitting, screened):
    picked = jnp.take(orbitals, points.astype(jnp.int32), axis=0)
    density = jnp.dot(picked, picked.T, preferred_element_type=jnp.float32)
    masked = (density * screened.astype(jnp.float32)).astype(jnp.bfloat16)
    applied = jnp.dot(masked, picked, preferred_element_type=jnp.float32).astype(jnp.bfloat16)
    exchange = -jnp.dot(applied.T, fitting.T, preferred_element_type=jnp.float32)
    rounded = exchange.astype(jnp.bfloat16)
    summed = jnp.dot(rounded, orbitals, preferred_element_type=jnp.float32)
    matrix = summed / math.sqrt(NR)
    return (exchange, matrix)
```

```python
import math

import jax
import jax.numpy as jnp
from jax import lax
from jax.sharding import Mesh, PartitionSpec as P

BF = jnp.bfloat16
F32 = jnp.float32
ORB = ("y", "xh", "core")
PLANE = ("y", "xh", "core", "pts")


def sent_to_all(x, axis):
    copies = jnp.broadcast_to(x, (lax.axis_size(axis), *x.shape))
    return lax.all_to_all(copies, axis, split_axis=0, concat_axis=0, tiled=True)


def per_device(orbitals, points, fitting, screened):
    n_grid = lax.axis_size("grid")
    n_plane = lax.axis_size(PLANE)
    grid_index = lax.axis_index("grid")
    plane_index = lax.axis_index(PLANE)
    rows_dev, width_dev = orbitals.shape
    nrows = rows_dev * n_grid
    nfull = width_dev * lax.axis_size(ORB)
    npoints = points.shape[0]
    row_block = npoints // n_plane
    column_block = npoints // n_grid
    share = nfull // (n_plane * n_grid)

    columns = sent_to_all(orbitals, "grid").reshape(nrows, width_dev)
    whole = lax.all_gather(columns, ORB, axis=1, tiled=True)
    fitted = sent_to_all(fitting, "grid").reshape(nrows, row_block)

    own = lax.dynamic_slice_in_dim(points, plane_index * row_block, row_block, 0)
    block = lax.dynamic_slice_in_dim(points, grid_index * column_block, column_block, 0)
    wanted = jnp.concatenate([own, block])
    rows = lax.broadcasted_iota(jnp.int32, (1, nrows), 1)
    choose = (wanted[:, None] == rows).astype(BF)
    picked = jnp.dot(choose, whole, preferred_element_type=F32).astype(BF)
    own_full, block_full = picked[:row_block], picked[row_block:]

    density = lax.dot_general(
        own_full, block_full, (((1,), (1,)), ((), ())), preferred_element_type=F32
    )
    masked = (density * screened.astype(F32)).astype(BF)
    partial = lax.dot_general(
        block_full, masked, (((0,), (1,)), ((), ())), preferred_element_type=F32
    ).astype(BF)
    partial = partial.reshape(n_plane, n_grid, share, row_block).transpose(1, 0, 2, 3)
    parts = lax.all_to_all(partial, "grid", 0, 0, tiled=True)
    applied = jnp.sum(parts.astype(F32), axis=0).astype(BF)
    applied = applied.reshape(n_plane * share, row_block)

    terms = lax.dot_general(
        applied, fitted, (((1,), (1,)), ((), ())), preferred_element_type=F32
    ).astype(BF)
    parts = lax.all_to_all(
        terms.reshape(n_plane, share, nrows), PLANE, 0, 0, tiled=True
    )
    exchange = -jnp.sum(parts.astype(F32), axis=0)
    matrix = jnp.dot(
        exchange.astype(BF), whole, preferred_element_type=F32
    ) / math.sqrt(nrows)
    both = jnp.stack(
        [exchange.reshape(share, n_grid, -1), matrix.reshape(share, n_grid, -1)]
    ).transpose(2, 0, 1, 3)
    both = lax.all_to_all(both, "grid", 0, 0, tiled=True)
    both = both.transpose(1, 0, 2, 3).reshape(2, n_grid * share, -1)
    return both[0], both[1]


def solution(mesh):
    n_grid, n_orb, n_pts = (mesh.shape[a] for a in ("grid", "orb", "pts"))
    fine = Mesh(
        mesh.devices.reshape(n_grid, n_orb // 4, 2, 2, n_pts),
        ("grid", "y", "xh", "core", "pts"),
    )
    in_specs = (P("grid", ORB), P(), P("grid", PLANE), P(PLANE, "grid"))
    out_specs = (P(PLANE, "grid"), P(PLANE, "grid"))
    return jax.shard_map(
        per_device, mesh=fine, in_specs=in_specs, out_specs=out_specs, check_vma=False
    )
```

```python
import math

import jax
import jax.numpy as jnp
from jax import lax
from jax.experimental import pallas as pl
from jax.experimental.pallas import tpu as pltpu
from jax.sharding import Mesh, PartitionSpec as P

BF = jnp.bfloat16
F32 = jnp.float32
ORB = ("y", "xh", "core")
PLANE = ("y", "xh", "core", "pts")
CHIPS = ("y", "xh", "pts")
X = ("xh", "pts")


def sent_to_all(x, axis):
    copies = jnp.broadcast_to(x, (lax.axis_size(axis), *x.shape))
    return lax.all_to_all(copies, axis, split_axis=0, concat_axis=0, tiled=True)


def from_next(x, step):
    n = lax.axis_size("y")
    return lax.ppermute(x, "y", [(i, (i - step) % n) for i in range(n)])


def along_y(x):
    half = x.shape[0] // 2
    after, before = from_next(x, 1), from_next(x, -1)
    far = (from_next(after[:half], 1), from_next(before[half:], -1))
    return x, after, far, before


def with_twin(x):
    return lax.ppermute(x, X, [(0, 1), (1, 0), (2, 3), (3, 2)])


def with_mirror(x):
    return lax.ppermute(x, X, [(0, 3), (3, 0), (1, 2), (2, 1)])


def along_x(x):
    half = x.shape[0] // 2
    twin, mirror = with_twin(x), with_mirror(x)
    far = (with_twin(mirror[:half]), with_mirror(twin[half:]))
    return x, twin, mirror, far


def other_core(x):
    return lax.ppermute(x, "core", [(0, 1), (1, 0)])


def pick_kernel(wanted_ref, ids_ref, *refs):
    pieces, (density_ref, picked_ref, columns_ref, choose_ref) = refs[:-4], refs[-4:]
    step = pl.program_id(0)
    rows = density_ref.shape[0]

    @pl.when(step == 0)
    def _():
        choose_ref[...] = (wanted_ref[...] == ids_ref[...]).astype(F32).astype(BF)
        density_ref[...] = jnp.zeros_like(density_ref)

    for k, piece in enumerate(pieces):
        width = piece.shape[-1]
        tall = piece.shape[-2]
        k_row, k_col = divmod(k, 2)
        columns_ref[0, k_row * tall : (k_row + 1) * tall, k_col * width : (k_col + 1) * width] = piece[0]
    picked = jnp.dot(choose_ref[...], columns_ref[0], preferred_element_type=F32).astype(BF)
    picked_ref[...] = picked[rows:]
    density_ref[...] += lax.dot_general(
        picked[:rows], picked[rows:], (((1,), (1,)), ((), ())), preferred_element_type=F32
    )


def pick(wanted, ids, pieces, rows):
    n, height, width = pieces[0].shape
    nrows = ids.shape[1]
    total = wanted.shape[0]
    rest = total - rows
    whole = lambda i: (0, 0)
    return pl.pallas_call(
        pick_kernel,
        grid=(n,),
        in_specs=[pl.BlockSpec((total, 1), whole), pl.BlockSpec((1, nrows), whole)]
        + [pl.BlockSpec((1, height, width), lambda i: (i, 0, 0))] * len(pieces),
        out_specs=[
            pl.BlockSpec((rows, rest), whole),
            pl.BlockSpec((rest, 2 * width), lambda i: (0, i)),
            pl.BlockSpec((1, nrows, 2 * width), lambda i: (i, 0, 0)),
        ],
        out_shape=[
            jax.ShapeDtypeStruct((rows, rest), F32),
            jax.ShapeDtypeStruct((rest, n * 2 * width), BF),
            jax.ShapeDtypeStruct((n, nrows, 2 * width), BF),
        ],
        scratch_shapes=[pltpu.VMEM((total, nrows), BF)],
        compiler_params=pltpu.CompilerParams(dimension_semantics=("arbitrary",)),
        cost_estimate=pl.CostEstimate(
            flops=2 * n * 2 * width * (total * nrows + rows * rest),
            bytes_accessed=2 * n * nrows * 4 * width,
            transcendentals=0,
        ),
        name="pick",
    )(wanted, ids, *pieces)


def per_device(orbitals, points, fitting, screened):
    n_grid = lax.axis_size("grid")
    n_plane = lax.axis_size(PLANE)
    grid_index = lax.axis_index("grid")
    plane_index = lax.axis_index(PLANE)
    y, xh, core, pts = (lax.axis_index(a) for a in PLANE)
    rows_dev, width = orbitals.shape
    nrows = rows_dev * n_grid
    nfull = width * lax.axis_size(ORB)
    npoints = points.shape[0]
    row_block = npoints // n_plane
    column_block = npoints // n_grid
    share = nfull // (n_plane * n_grid)
    part = rows_dev // 2
    quarter = nrows // 4

    own_rows = lax.dynamic_slice_in_dim(orbitals, pts * part, part, 0)
    held = sent_to_all(own_rows, "grid").reshape(2, quarter, width)
    alpha, beta = held[0], held[1]
    a0, a1, a2, a3 = along_y(alpha)
    b0, b1, b2, b3 = along_x(beta)
    a_own, a_twin, a_mirror, a_far = along_x(jnp.stack([a0, a1, jnp.concatenate(a2), a3]))
    b_all = along_y(jnp.stack([b0, b1, b2, jnp.concatenate(b3)]))
    a_far = jnp.concatenate(a_far)
    b_all = [jnp.concatenate(b) if isinstance(b, tuple) else b for b in b_all]
    b_own, b_twin, b_mirror, b_far = (jnp.stack([b[k] for b in b_all]) for k in range(4))

    fit_own = sent_to_all(fitting, "grid").reshape(nrows, row_block)
    fit_other = other_core(fit_own)

    near = lax.broadcasted_iota(jnp.int32, (nrows,), 0)
    half_of = lax.rem(near // (nrows // 2) + pts, 2)
    within = lax.rem(near, nrows // 2)
    ids = (within // part) * rows_dev + half_of * part + lax.rem(within, part)
    mine = lax.dynamic_slice_in_dim(points, plane_index * row_block, row_block, 0)
    theirs_index = plane_index + (1 - 2 * core) * lax.axis_size("pts")
    theirs = lax.dynamic_slice_in_dim(points, theirs_index * row_block, row_block, 0)
    block = lax.dynamic_slice_in_dim(points, grid_index * column_block, column_block, 0)
    wanted = jnp.concatenate([mine, theirs, block])
    wanted, fit_own, fit_other = lax.optimization_barrier((wanted, fit_own, fit_other))
    density, picked, columns = pick(
        wanted[:, None],
        ids[None],
        [a_own, a_far, b_own, b_far, a_twin, a_mirror, b_twin, b_mirror],
        2 * row_block,
    )

    density = density[:row_block] + other_core(density[row_block:])
    masked = (density * screened.astype(F32)).astype(BF)
    masked_other = other_core(masked)

    def applied_by(masked):
        partial = lax.dot_general(
            picked, masked, (((0,), (1,)), ((), ())), preferred_element_type=F32
        ).astype(BF)
        partial = partial.reshape(-1, n_grid, share, row_block)
        return partial.transpose(1, 0, 2, 3)

    partial = jnp.stack([applied_by(masked), applied_by(masked_other)], axis=1)
    parts = lax.all_to_all(partial, "grid", 0, 0, tiled=True)
    applied = jnp.sum(parts.astype(F32), axis=0).astype(BF)
    applied = applied.reshape(2, 4, 2, 2 * share, row_block)
    applied = jnp.where(xh == 0, applied, applied[:, :, ::-1])
    applied = lax.dynamic_slice_in_dim(
        jnp.concatenate([applied, applied], axis=1), lax.rem(4 - y, 4), 4, 1
    ).reshape(2, -1, row_block)
    terms = sum(
        lax.dot_general(a, f, (((1,), (1,)), ((), ())), preferred_element_type=F32)
        for a, f in ((applied[0], fit_own), (applied[1], fit_other))
    ).astype(BF)
    parts = lax.all_to_all(terms.reshape(-1, share, nrows), CHIPS, 0, 0, tiled=True)
    exchange = -jnp.sum(parts.astype(F32), axis=0)
    exchange = jnp.stack([exchange, other_core(exchange)])
    exchange = jnp.where(core == 0, exchange, exchange[::-1])

    halves = exchange.astype(BF).reshape(2 * share, n_grid, 2, part)
    halves = jnp.where(pts == 0, halves, halves[:, :, ::-1])
    halves = halves.transpose(0, 2, 1, 3).reshape(2 * share, nrows)
    matrix = lax.dot_general(
        halves, columns, (((1,), (1,)), ((), ())), preferred_element_type=F32
    ) / math.sqrt(nrows)
    matrix = matrix.transpose(1, 0, 2).reshape(4, 2 * share, 2, width).transpose(0, 2, 1, 3)
    matrix = jnp.where(xh == 0, matrix, matrix[:, ::-1])
    matrix = lax.dynamic_slice_in_dim(
        jnp.concatenate([matrix, matrix]), lax.rem(4 - y, 4), 4, 0
    ).reshape(n_grid, 2, share, width)
    mine = exchange.reshape(2, share, n_grid, 2, width)
    mine = lax.dynamic_index_in_dim(mine, core, 3, keepdims=False).transpose(2, 0, 1, 3)
    both = jnp.stack([mine, matrix], axis=2).reshape(2 * n_grid, 2, share, width)
    both = lax.all_to_all(both, ("grid", "core"), 0, 0, tiled=True)
    both = both.reshape(n_grid, 2, 2, share, width).transpose(2, 0, 3, 1, 4)
    both = both.reshape(2, n_grid * share, 2 * width)
    return both[0], both[1]


def solution(mesh):
    n_grid, n_orb, n_pts = (mesh.shape[a] for a in ("grid", "orb", "pts"))
    fine = Mesh(
        mesh.devices.reshape(n_grid, n_orb // 4, 2, 2, n_pts),
        ("grid", "y", "xh", "core", "pts"),
    )
    in_specs = (P("grid", ORB), P(), P("grid", PLANE), P(PLANE, "grid"))
    out_specs = (P(PLANE, "grid"), P(PLANE, "grid"))
    return jax.shard_map(
        per_device, mesh=fine, in_specs=in_specs, out_specs=out_specs, check_vma=False
    )
```

```python
import math

import jax
import jax.numpy as jnp
from jax import lax
from jax.experimental import pallas as pl
from jax.experimental.pallas import tpu as pltpu
from jax.sharding import Mesh, PartitionSpec as P


BF = jnp.bfloat16
F32 = jnp.float32
ORB = ("y", "xh", "core")
PLANE = ("y", "xh", "core", "pts")
CHIPS = ("y", "xh", "pts")
X = ("xh", "pts")


def sent_to_all(x, axis):
    copies = jnp.broadcast_to(x, (lax.axis_size(axis), *x.shape))
    return lax.all_to_all(copies, axis, split_axis=0, concat_axis=0, tiled=True)


def from_next(x, step):
    n = lax.axis_size("y")
    return lax.ppermute(x, "y", [(i, (i - step) % n) for i in range(n)])


def with_twin(x):
    return lax.ppermute(x, X, [(0, 1), (1, 0), (2, 3), (3, 2)])


def with_mirror(x):
    return lax.ppermute(x, X, [(0, 3), (3, 0), (1, 2), (2, 1)])


def with_far(x):
    return lax.ppermute(x, X, [(0, 2), (2, 0), (1, 3), (3, 1)])


def along_y(first, second):
    after, before = from_next(first, 1), from_next(first, -1)
    after2, before2 = from_next(second, 1), from_next(second, -1)
    far, far2 = from_next(after, 1), from_next(before2, -1)
    return (first, after, far, before), (second, after2, far2, before2)


def along_x(first, second):
    twin, mirror = with_twin(first), with_mirror(first)
    twin2, mirror2 = with_twin(second), with_mirror(second)
    far, far2 = with_twin(mirror), with_mirror(twin2)
    return (first, twin, mirror, far), (second, twin2, mirror2, far2)


def other_core(x):
    return lax.ppermute(x, "core", [(0, 1), (1, 0)])


def pick_kernel(choose_ref, *refs):
    pieces, outs = refs[:-4], refs[-4:]
    own_ref, other_ref, picked_ref, columns_ref = outs
    step = pl.program_id(0)
    rows = own_ref.shape[0]
    height, width = pieces[0].shape[1:]
    alpha, beta = pieces[:8], pieces[8:]

    @pl.when(step == 0)
    def _():
        own_ref[...] = jnp.zeros_like(own_ref)
        other_ref[...] = jnp.zeros_like(other_ref)

    for at in range(4):

        @pl.when(step == at)
        def _():
            for col, roles in enumerate(((0, 1), (3, 2))):
                for k, role in enumerate(roles):
                    for part, piece in enumerate(
                        (alpha[role + 4 * (at // 2)][at % 2], beta[at + 4 * (role // 2)][role % 2])
                    ):
                        top = (2 * k + part) * height
                        columns_ref[0, top : top + height, col * width : (col + 1) * width] = piece

    picked = jnp.dot(choose_ref[...], columns_ref[0], preferred_element_type=F32).astype(BF)
    picked_ref[...] = picked[2 * rows :]
    for k, out in enumerate((own_ref, other_ref)):
        out[...] += lax.dot_general(
            picked[k * rows : (k + 1) * rows],
            picked[2 * rows :],
            (((1,), (1,)), ((), ())),
            preferred_element_type=F32,
        )


def pick(choose, pieces, rows):
    _, height, width = pieces[0].shape
    total, nrows = choose.shape
    rest = total - 2 * rows
    whole = lambda i: (0, 0)
    return pl.pallas_call(
        pick_kernel,
        grid=(4,),
        in_specs=[pl.BlockSpec((total, nrows), whole)]
        + [pl.BlockSpec((2, height, width), lambda i: (0, 0, 0))] * len(pieces),
        out_specs=[
            pl.BlockSpec((rows, rest), whole),
            pl.BlockSpec((rows, rest), whole),
            pl.BlockSpec((rest, 2 * width), lambda i: (0, i)),
            pl.BlockSpec((1, nrows, 2 * width), lambda i: (i, 0, 0)),
        ],
        out_shape=[
            jax.ShapeDtypeStruct((rows, rest), F32),
            jax.ShapeDtypeStruct((rows, rest), F32),
            jax.ShapeDtypeStruct((rest, 8 * width), BF),
            jax.ShapeDtypeStruct((4, nrows, 2 * width), BF),
        ],
        compiler_params=pltpu.CompilerParams(dimension_semantics=("arbitrary",), vmem_limit_bytes=30 << 20),
        cost_estimate=pl.CostEstimate(
            flops=16 * width * (total * nrows + 2 * rows * rest),
            bytes_accessed=16 * nrows * width,
            transcendentals=0,
        ),
        name="pick",
    )(choose, *pieces)


def body(orbitals, points, fitting, screened):
    n_grid = lax.axis_size("grid")
    n_plane = lax.axis_size(PLANE)
    grid_index = lax.axis_index("grid")
    plane_index = lax.axis_index(PLANE)
    y, xh, core, pts = (lax.axis_index(a) for a in PLANE)
    rows_dev, width = orbitals.shape
    nrows = rows_dev * n_grid
    nfull = width * lax.axis_size(ORB)
    npoints = points.shape[0]
    row_block = npoints // n_plane
    column_block = npoints // n_grid
    share = nfull // (n_plane * n_grid)
    part = rows_dev // 2
    quarter = nrows // 4

    own_rows = lax.dynamic_slice_in_dim(orbitals, pts * part, part, 0)
    held = sent_to_all(own_rows, "grid").reshape(2, quarter, width)
    alpha, beta = held[0], held[1]
    alphas = [alpha, from_next(alpha, 1), from_next(alpha, 2), from_next(alpha, -1)]
    betas = [beta, with_twin(beta), with_mirror(beta), with_far(beta)]
    a_first, a_second = jnp.stack(alphas[:2]), jnp.stack(alphas[2:])
    b_first, b_second = jnp.stack(betas[:2]), jnp.stack(betas[2:])
    pieces = [x for part in along_x(a_first, a_second) + along_y(b_first, b_second) for x in part]

    fit_own = sent_to_all(fitting, "grid").reshape(nrows, row_block)
    fit_other = other_core(fit_own)

    near = lax.broadcasted_iota(jnp.int32, (nrows,), 0)
    half_of = lax.rem(near // (nrows // 2) + pts, 2)
    within = lax.rem(near, nrows // 2)
    ids = (within // part) * rows_dev + half_of * part + lax.rem(within, part)
    mine = lax.dynamic_slice_in_dim(points, plane_index * row_block, row_block, 0)
    theirs_index = plane_index + (1 - 2 * core) * lax.axis_size("pts")
    theirs = lax.dynamic_slice_in_dim(points, theirs_index * row_block, row_block, 0)
    block = lax.dynamic_slice_in_dim(points, grid_index * column_block, column_block, 0)
    wanted = jnp.concatenate([mine, theirs, block])
    choose = (wanted[:, None] == ids[None]).astype(BF)
    density, density_other, picked, columns = pick(choose, pieces, row_block)

    density = density + other_core(density_other)
    masked = (density * screened.astype(F32)).astype(BF)
    masked, fit_own = lax.optimization_barrier((masked, fit_own))
    masked_other = other_core(masked)

    def applied_by(masked):
        partial = lax.dot_general(
            picked, masked, (((0,), (1,)), ((), ())), preferred_element_type=F32
        ).astype(BF)
        partial = partial.reshape(-1, n_grid, share, row_block)
        return partial.transpose(1, 0, 2, 3)

    partial = jnp.stack([applied_by(masked), applied_by(masked_other)], axis=1)
    parts = lax.all_to_all(partial, "grid", 0, 0, tiled=True)
    applied = jnp.sum(parts.astype(F32), axis=0).astype(BF)
    applied = applied.reshape(2, 4, 2, 2 * share, row_block)
    applied = jnp.where(xh == 0, applied, applied[:, :, ::-1])
    applied = lax.dynamic_slice_in_dim(
        jnp.concatenate([applied, applied], axis=1), lax.rem(4 - y, 4), 4, 1
    ).reshape(2, -1, row_block)
    terms = sum(
        lax.dot_general(a, f, (((1,), (1,)), ((), ())), preferred_element_type=F32)
        for a, f in ((applied[0], fit_own), (applied[1], fit_other))
    ).astype(BF)
    parts = lax.all_to_all(terms.reshape(-1, share, nrows), CHIPS, 0, 0, tiled=True)
    exchange = -jnp.sum(parts.astype(F32), axis=0)
    exchange = jnp.stack([exchange, other_core(exchange)])
    exchange = jnp.where(core == 0, exchange, exchange[::-1])

    halves = exchange.astype(BF).reshape(2 * share, n_grid, 2, part)
    halves = jnp.where(pts == 0, halves, halves[:, :, ::-1])
    halves = halves.transpose(0, 2, 1, 3).reshape(2 * share, nrows)
    matrix = lax.dot_general(
        halves, columns, (((1,), (1,)), ((), ())), preferred_element_type=F32
    ) / math.sqrt(nrows)
    matrix = matrix.transpose(1, 0, 2).reshape(4, 2 * share, 2, width).transpose(0, 2, 1, 3)
    matrix = jnp.where(xh == 0, matrix, matrix[:, ::-1])
    matrix = lax.dynamic_slice_in_dim(
        jnp.concatenate([matrix, matrix]), lax.rem(4 - y, 4), 4, 0
    ).reshape(n_grid, 2, share, width)
    mine = exchange.reshape(2, share, n_grid, 2, width)
    mine = lax.dynamic_index_in_dim(mine, core, 3, keepdims=False).transpose(2, 0, 1, 3)
    both = jnp.stack([mine, matrix], axis=2).reshape(2 * n_grid, 2, share, width)
    both = lax.all_to_all(both, ("grid", "core"), 0, 0, tiled=True)
    both = both.reshape(n_grid, 2, 2, share, width).transpose(2, 0, 3, 1, 4)
    both = both.reshape(2, n_grid * share, 2 * width)
    return both[0], both[1]


def solution(mesh):
    n_grid, n_orb, n_pts = (mesh.shape[a] for a in ("grid", "orb", "pts"))
    fine = Mesh(
        mesh.devices.reshape(n_grid, n_orb // 4, 2, 2, n_pts),
        ("grid", "y", "xh", "core", "pts"),
    )
    in_specs = (P("grid", ORB), P(), P("grid", PLANE), P(PLANE, "grid"))
    out_specs = (P(PLANE, "grid"), P(PLANE, "grid"))
    return jax.shard_map(body, mesh=fine, in_specs=in_specs, out_specs=out_specs, check_vma=False)
```

```python
import math

import jax
import jax.numpy as jnp
from jax import lax
from jax.experimental import pallas as pl
from jax.experimental.pallas import tpu as pltpu
from jax.sharding import Mesh, PartitionSpec as P


BF = jnp.bfloat16
F32 = jnp.float32
ORB = ("y", "xh", "core")
PLANE = ("y", "xh", "core", "pts")
CHIPS = ("y", "xh", "pts")
X = ("xh", "pts")


def sent_to_all(x, axis):
    copies = jnp.broadcast_to(x, (lax.axis_size(axis), *x.shape))
    return lax.all_to_all(copies, axis, split_axis=0, concat_axis=0, tiled=True)


def from_next(x, step):
    n = lax.axis_size("y")
    return lax.ppermute(x, "y", [(i, (i - step) % n) for i in range(n)])


def with_twin(x):
    return lax.ppermute(x, X, [(0, 1), (1, 0), (2, 3), (3, 2)])


def with_mirror(x):
    return lax.ppermute(x, X, [(0, 3), (3, 0), (1, 2), (2, 1)])


def with_far(x):
    return lax.ppermute(x, X, [(0, 2), (2, 0), (1, 3), (3, 1)])


def along_y(first, second):
    after, before = from_next(first, 1), from_next(first, -1)
    after2, before2 = from_next(second, 1), from_next(second, -1)
    far, far2 = from_next(after, 1), from_next(before2, -1)
    return (first, after, far, before), (second, after2, far2, before2)


def along_x(first, second):
    twin, mirror = with_twin(first), with_mirror(first)
    twin2, mirror2 = with_twin(second), with_mirror(second)
    far, far2 = with_twin(mirror), with_mirror(twin2)
    return (first, twin, mirror, far), (second, twin2, mirror2, far2)


def other_core(x):
    return lax.ppermute(x, "core", [(0, 1), (1, 0)])


def pick_kernel(spots_ref, *refs):
    pieces, outs = refs[:16], refs[16:20]
    own_ref, other_ref, picked_ref, columns_out_ref = outs
    wide_ref, chosen_ref, rows_ref, columns_ref, sem = refs[20:]
    rows = own_ref.shape[0]
    rest = picked_ref.shape[0]
    height, width = pieces[0].shape[1:]
    alpha, beta = pieces[:8], pieces[8:]
    group = 256

    for at in range(4):
        for col, roles in enumerate(((0, 1), (3, 2))):
            for k, role in enumerate(roles):
                for part, (piece, which) in enumerate(
                    ((alpha[role + 4 * (at // 2)], at % 2), (beta[at + 4 * (role // 2)], role % 2))
                ):
                    top = (2 * k + part) * height

                    def spread(i, _, piece=piece, which=which, top=top, at=at, col=col):
                        start = pl.multiple_of(i * group, group)
                        block = piece[which, pl.ds(start, group), :]
                        columns_ref[at, pl.ds(top + start, group), col * width : (col + 1) * width] = block
                        wide_ref[pl.ds((top + start) * 8 + 2 * at + col, group, stride=8), :] = block.astype(F32)
                        return _

                    lax.fori_loop(0, height // group, spread, 0)

    keep = pltpu.make_async_copy(columns_ref, columns_out_ref, sem)
    keep.start()

    def choose(i, _):
        for k in range(16):
            spot = pl.multiple_of(spots_ref[i * 16 + k] * 8, 8)
            to = pl.multiple_of(i * 128 + k * 8, 8)
            chosen_ref[pl.ds(to, 8), :] = wide_ref[pl.ds(spot, 8), :]
        return _

    lax.fori_loop(0, (2 * rows + rest) // 16, choose, 0)

    for target, first, count in ((rows_ref, 0, 2 * rows), (picked_ref, 2 * rows, rest)):
        for k in range(8):

            def gather(i, _, target=target, first=first, k=k):
                start = pl.multiple_of(i * group, group)
                block = chosen_ref[pl.ds((first + start) * 8 + k, group, stride=8), :]
                target[pl.ds(start, group), k * width : (k + 1) * width] = block.astype(BF)
                return _

            lax.fori_loop(0, count // group, gather, 0)

    for k, out in enumerate((own_ref, other_ref)):
        out[...] = lax.dot_general(
            rows_ref[k * rows : (k + 1) * rows], picked_ref[...], (((1,), (1,)), ((), ())),
            preferred_element_type=F32)
    keep.wait()


def pick(spots, pieces, rows):
    _, height, width = pieces[0].shape
    total, nrows = spots.shape[0], 4 * height
    rest = total - 2 * rows
    vm = pl.BlockSpec(memory_space=pltpu.VMEM)
    return pl.pallas_call(
        pick_kernel,
        in_specs=[pl.BlockSpec(memory_space=pltpu.SMEM)] + [vm] * 16,
        out_specs=[vm] * 3 + [pl.BlockSpec(memory_space=pltpu.HBM)],
        out_shape=[
            jax.ShapeDtypeStruct((rows, rest), F32),
            jax.ShapeDtypeStruct((rows, rest), F32),
            jax.ShapeDtypeStruct((rest, 8 * width), BF),
            pltpu.HBM((4, nrows, 2 * width), BF),
        ],
        scratch_shapes=[
            pltpu.VMEM((nrows * 8, width), F32),
            pltpu.VMEM((total * 8, width), F32),
            pltpu.VMEM((2 * rows, 8 * width), BF),
            pltpu.VMEM((4, nrows, 2 * width), BF),
            pltpu.SemaphoreType.DMA,
        ],
        compiler_params=pltpu.CompilerParams(vmem_limit_bytes=26 << 20),
        cost_estimate=pl.CostEstimate(
            flops=4 * rows * rest * 8 * width, bytes_accessed=32 * nrows * width, transcendentals=0
        ),
        name="pick",
    )(spots, *pieces)


def body(orbitals, points, fitting, screened):
    n_grid = lax.axis_size("grid")
    n_plane = lax.axis_size(PLANE)
    grid_index = lax.axis_index("grid")
    plane_index = lax.axis_index(PLANE)
    y, xh, core, pts = (lax.axis_index(a) for a in PLANE)
    rows_dev, width = orbitals.shape
    nrows = rows_dev * n_grid
    nfull = width * lax.axis_size(ORB)
    npoints = points.shape[0]
    row_block = npoints // n_plane
    column_block = npoints // n_grid
    share = nfull // (n_plane * n_grid)
    part = rows_dev // 2
    quarter = nrows // 4

    own_rows = lax.dynamic_slice_in_dim(orbitals, pts * part, part, 0)
    held = sent_to_all(own_rows, "grid").reshape(2, quarter, width)
    alpha, beta = held[0], held[1]
    alphas = [alpha, from_next(alpha, 1), from_next(alpha, 2), from_next(alpha, -1)]
    betas = [beta, with_twin(beta), with_mirror(beta), with_far(beta)]
    a_first, a_second = jnp.stack(alphas[:2]), jnp.stack(alphas[2:])
    b_first, b_second = jnp.stack(betas[:2]), jnp.stack(betas[2:])
    pieces = [x for part in along_x(a_first, a_second) + along_y(b_first, b_second) for x in part]

    copies = jnp.broadcast_to(fitting, (n_grid, *fitting.shape))
    fit_own = lax.all_to_all(copies, "grid", 0, 0, tiled=True).reshape(nrows, row_block)
    fit_other = other_core(fit_own)

    mine = lax.dynamic_slice_in_dim(points, plane_index * row_block, row_block, 0)
    theirs_index = plane_index + (1 - 2 * core) * lax.axis_size("pts")
    theirs = lax.dynamic_slice_in_dim(points, theirs_index * row_block, row_block, 0)
    block = lax.dynamic_slice_in_dim(points, grid_index * column_block, column_block, 0)
    wanted = jnp.concatenate([mine, theirs, block])
    half_of = lax.rem(wanted, rows_dev) // part
    spots = (half_of ^ pts) * (nrows // 2) + wanted // rows_dev * part + lax.rem(wanted, part)
    density, density_other, picked, columns = pick(spots, pieces, row_block)

    density = density + other_core(density_other)
    masked = (density * screened.astype(F32)).astype(BF)
    masked, fit_own = lax.optimization_barrier((masked, fit_own))
    masked_other = other_core(masked)

    def applied_by(masked):
        partial = lax.dot_general(
            picked, masked, (((0,), (1,)), ((), ())), preferred_element_type=F32
        ).astype(BF)
        partial = partial.reshape(-1, n_grid, share, row_block)
        return partial.transpose(1, 0, 2, 3)

    partial = jnp.stack([applied_by(masked), applied_by(masked_other)], axis=1)
    parts = lax.all_to_all(partial, "grid", 0, 0, tiled=True)
    applied = jnp.sum(parts.astype(F32), axis=0).astype(BF)
    applied = applied.reshape(2, 4, 2, 2 * share, row_block)
    applied = jnp.where(xh == 0, applied, applied[:, :, ::-1])
    applied = lax.dynamic_slice_in_dim(
        jnp.concatenate([applied, applied], axis=1), lax.rem(4 - y, 4), 4, 1
    ).reshape(2, -1, row_block)
    terms = sum(
        lax.dot_general(a, f, (((1,), (1,)), ((), ())), preferred_element_type=F32)
        for a, f in ((applied[0], fit_own), (applied[1], fit_other))
    ).astype(BF)
    parts = lax.all_to_all(terms.reshape(-1, share, nrows), CHIPS, 0, 0, tiled=True)
    exchange = -jnp.sum(parts.astype(F32), axis=0)
    exchange = jnp.stack([exchange, other_core(exchange)])
    exchange = jnp.where(core == 0, exchange, exchange[::-1])

    halves = exchange.astype(BF).reshape(2 * share, n_grid, 2, part)
    halves = jnp.where(pts == 0, halves, halves[:, :, ::-1])
    halves = halves.transpose(0, 2, 1, 3).reshape(2 * share, nrows)
    matrix = lax.dot_general(
        halves, columns, (((1,), (1,)), ((), ())), preferred_element_type=F32
    ) / math.sqrt(nrows)
    matrix = matrix.transpose(1, 0, 2).reshape(4, 2 * share, 2, width).transpose(0, 2, 1, 3)
    matrix = jnp.where(xh == 0, matrix, matrix[:, ::-1])
    matrix = lax.dynamic_slice_in_dim(
        jnp.concatenate([matrix, matrix]), lax.rem(4 - y, 4), 4, 0
    ).reshape(n_grid, 2, share, width)
    mine = exchange.reshape(2, share, n_grid, 2, width)
    mine = lax.dynamic_index_in_dim(mine, core, 3, keepdims=False).transpose(2, 0, 1, 3)
    both = jnp.stack([mine, matrix], axis=2).reshape(2 * n_grid, 2, share, width)
    both = lax.all_to_all(both, ("grid", "core"), 0, 0, tiled=True)
    both = both.reshape(n_grid, 2, 2, share, width).transpose(2, 0, 3, 1, 4)
    both = both.reshape(2, n_grid * share, 2 * width)
    return both[0], both[1]


def solution(mesh):
    n_grid, n_orb, n_pts = (mesh.shape[a] for a in ("grid", "orb", "pts"))
    fine = Mesh(
        mesh.devices.reshape(n_grid, n_orb // 4, 2, 2, n_pts),
        ("grid", "y", "xh", "core", "pts"),
    )
    in_specs = (P("grid", ORB), P(), P("grid", PLANE), P(PLANE, "grid"))
    out_specs = (P(PLANE, "grid"), P(PLANE, "grid"))
    return jax.shard_map(body, mesh=fine, in_specs=in_specs, out_specs=out_specs, check_vma=False)
```

```python
import math

import jax
import jax.numpy as jnp
from jax import lax
from jax.experimental import pallas as pl
from jax.experimental.pallas import tpu as pltpu
from jax.sharding import Mesh, PartitionSpec as P


BF = jnp.bfloat16
F32 = jnp.float32
ORB = ("y", "xh", "core")
PLANE = ("y", "xh", "core", "pts")
CHIPS = ("y", "xh", "pts")
X = ("xh", "pts")


def sent_to_all(x, axis):
    copies = jnp.broadcast_to(x, (lax.axis_size(axis), *x.shape))
    return lax.all_to_all(copies, axis, split_axis=0, concat_axis=0, tiled=True)


def from_next(x, step):
    n = lax.axis_size("y")
    return lax.ppermute(x, "y", [(i, (i - step) % n) for i in range(n)])


def with_twin(x):
    return lax.ppermute(x, X, [(0, 1), (1, 0), (2, 3), (3, 2)])


def with_mirror(x):
    return lax.ppermute(x, X, [(0, 3), (3, 0), (1, 2), (2, 1)])


def with_far(x):
    return lax.ppermute(x, X, [(0, 2), (2, 0), (1, 3), (3, 1)])


def along_y(first, second):
    after, before = from_next(first, 1), from_next(first, -1)
    after2, before2 = from_next(second, 1), from_next(second, -1)
    far, far2 = from_next(after, 1), from_next(before2, -1)
    return (first, after, far, before), (second, after2, far2, before2)


def along_x(first, second):
    twin, mirror = with_twin(first), with_mirror(first)
    twin2, mirror2 = with_twin(second), with_mirror(second)
    far, far2 = with_twin(mirror), with_mirror(twin2)
    return (first, twin, mirror, far), (second, twin2, mirror2, far2)


def other_core(x):
    return lax.ppermute(x, "core", [(0, 1), (1, 0)])


def pick_kernel(spots_ref, *refs):
    pieces, outs = refs[:16], refs[16:20]
    own_ref, other_ref, picked_ref, columns_out_ref = outs
    wide_ref, chosen_ref, rows_ref, columns_ref, sem = refs[20:]
    rows = own_ref.shape[0]
    rest = picked_ref.shape[0]
    height, width = pieces[0].shape[1:]
    alpha, beta = pieces[:8], pieces[8:]
    group = 256

    for at in range(4):
        for col, roles in enumerate(((0, 1), (3, 2))):
            for k, role in enumerate(roles):
                for part, (piece, which) in enumerate(
                    ((alpha[role + 4 * (at // 2)], at % 2), (beta[at + 4 * (role // 2)], role % 2))
                ):
                    top = (2 * k + part) * height

                    def spread(i, _, piece=piece, which=which, top=top, at=at, col=col):
                        start = pl.multiple_of(i * group, group)
                        block = piece[which, pl.ds(start, group), :]
                        columns_ref[at, pl.ds(top + start, group), col * width : (col + 1) * width] = block
                        wide_ref[pl.ds((top + start) * 8 + 2 * at + col, group, stride=8), :] = block.astype(F32)
                        return _

                    lax.fori_loop(0, height // group, spread, 0)

    keep = pltpu.make_async_copy(columns_ref, columns_out_ref, sem)
    keep.start()

    def choose(i, _):
        for k in range(16):
            spot = pl.multiple_of(spots_ref[i * 16 + k] * 8, 8)
            to = pl.multiple_of(i * 128 + k * 8, 8)
            chosen_ref[pl.ds(to, 8), :] = wide_ref[pl.ds(spot, 8), :]
        return _

    lax.fori_loop(0, (2 * rows + rest) // 16, choose, 0)

    for target, first, count in ((rows_ref, 0, 2 * rows), (picked_ref, 2 * rows, rest)):
        for k in range(8):

            def gather(i, _, target=target, first=first, k=k):
                start = pl.multiple_of(i * group, group)
                block = chosen_ref[pl.ds((first + start) * 8 + k, group, stride=8), :]
                target[pl.ds(start, group), k * width : (k + 1) * width] = block.astype(BF)
                return _

            lax.fori_loop(0, count // group, gather, 0)

    for k, out in enumerate((own_ref, other_ref)):
        out[...] = lax.dot_general(
            rows_ref[k * rows : (k + 1) * rows], picked_ref[...], (((1,), (1,)), ((), ())),
            preferred_element_type=F32)
    keep.wait()


def pick(spots, pieces, rows):
    _, height, width = pieces[0].shape
    total, nrows = spots.shape[0], 4 * height
    rest = total - 2 * rows
    vm = pl.BlockSpec(memory_space=pltpu.VMEM)
    return pl.pallas_call(
        pick_kernel,
        in_specs=[pl.BlockSpec(memory_space=pltpu.SMEM)] + [vm] * 16,
        out_specs=[vm] * 3 + [pl.BlockSpec(memory_space=pltpu.HBM)],
        out_shape=[
            jax.ShapeDtypeStruct((rows, rest), F32),
            jax.ShapeDtypeStruct((rows, rest), F32),
            jax.ShapeDtypeStruct((rest, 8 * width), BF),
            pltpu.HBM((4, nrows, 2 * width), BF),
        ],
        scratch_shapes=[
            pltpu.VMEM((nrows * 8, width), F32),
            pltpu.VMEM((total * 8, width), F32),
            pltpu.VMEM((2 * rows, 8 * width), BF),
            pltpu.VMEM((4, nrows, 2 * width), BF),
            pltpu.SemaphoreType.DMA,
        ],
        compiler_params=pltpu.CompilerParams(vmem_limit_bytes=26 << 20),
        cost_estimate=pl.CostEstimate(
            flops=4 * rows * rest * 8 * width, bytes_accessed=32 * nrows * width, transcendentals=0
        ),
        name="pick",
    )(spots, *pieces)


def apply_kernel(place_ref, picked_ref, own_ref, other_ref, *refs):
    outs, held_ref = refs[:-1], refs[-1]
    rows = own_ref.shape[0]
    groups, n, share, _ = held_ref.shape
    for k, ref in enumerate((own_ref, other_ref)):
        product = jnp.dot(ref[...], picked_ref[...], preferred_element_type=F32)
        held_ref[:, :, :, k * rows : (k + 1) * rows] = product.T.reshape(groups, n, share, rows)
    for k, out in enumerate(outs[:n]):
        if k == n // 2:
            half = groups // 2
            spot = lax.rem(place_ref[0] + k, n)
            out[...] = held_ref[:half, spot].astype(BF)
            outs[n][...] = held_ref[half:, spot].astype(BF)
        else:
            out[...] = held_ref[:, lax.rem(place_ref[0] + k, n)].astype(BF)


def applied_shares(place, picked, own, other, n, share):
    rows, columns = own.shape[0], picked.shape[1]
    groups = columns // (n * share)
    vm = pl.BlockSpec(memory_space=pltpu.VMEM)
    counts = [groups] * n + [groups // 2]
    counts[n // 2] = groups // 2
    return pl.pallas_call(
        apply_kernel,
        in_specs=[pl.BlockSpec(memory_space=pltpu.SMEM)] + [vm] * 3,
        out_specs=[vm] * (n + 1),
        out_shape=[jax.ShapeDtypeStruct((c, share, 2 * rows), BF) for c in counts],
        scratch_shapes=[pltpu.VMEM((groups, n, share, 2 * rows), F32)],
        compiler_params=pltpu.CompilerParams(vmem_limit_bytes=16 << 20),
        cost_estimate=pl.CostEstimate(
            flops=4 * rows * columns * own.shape[1], bytes_accessed=8 * rows * columns, transcendentals=0
        ),
        name="applied",
    )(place, picked, own, other)


def to_grid(x, step):
    n = lax.axis_size("grid")
    return lax.ppermute(x, "grid", [(i, (i + step) % n) for i in range(n)])


def summed_on_grid(shares):
    total = shares[0].astype(F32)
    opposite = {1: shares[4], -1: shares[8]}
    near = {1: shares[1], -1: shares[7]}
    second = {1: shares[2], -1: shares[6]}
    third = {1: shares[3], -1: shares[5]}
    opposite = {way: to_grid(x, 3 * way) for way, x in opposite.items()}
    third = {way: to_grid(x, 2 * way) for way, x in third.items()}
    second = {way: to_grid(x, way) for way, x in second.items()}
    sums = []
    for way in (1, -1):
        none = jnp.zeros_like(opposite[way])
        both = [opposite[way], none] if way == 1 else [none, opposite[way]]
        terms = near[way], second[way], third[way], jnp.concatenate(both)
        sums.append(to_grid(sum(t.astype(F32) for t in terms).astype(BF), way))
    return (total + sums[0].astype(F32) + sums[1].astype(F32)).astype(BF)


def body(orbitals, points, fitting, screened):
    n_grid = lax.axis_size("grid")
    n_plane = lax.axis_size(PLANE)
    grid_index = lax.axis_index("grid")
    plane_index = lax.axis_index(PLANE)
    y, xh, core, pts = (lax.axis_index(a) for a in PLANE)
    rows_dev, width = orbitals.shape
    nrows = rows_dev * n_grid
    nfull = width * lax.axis_size(ORB)
    npoints = points.shape[0]
    row_block = npoints // n_plane
    column_block = npoints // n_grid
    share = nfull // (n_plane * n_grid)
    part = rows_dev // 2
    quarter = nrows // 4

    own_rows = lax.dynamic_slice_in_dim(orbitals, pts * part, part, 0)
    held = sent_to_all(own_rows, "grid").reshape(2, quarter, width)
    alpha, beta = held[0], held[1]
    alphas = [alpha, from_next(alpha, 1), from_next(alpha, 2), from_next(alpha, -1)]
    betas = [beta, with_twin(beta), with_mirror(beta), with_far(beta)]
    a_first, a_second = jnp.stack(alphas[:2]), jnp.stack(alphas[2:])
    b_first, b_second = jnp.stack(betas[:2]), jnp.stack(betas[2:])
    pieces = [x for part in along_x(a_first, a_second) + along_y(b_first, b_second) for x in part]

    copies = jnp.broadcast_to(fitting, (n_grid, *fitting.shape))
    fit_own = lax.all_to_all(copies, "grid", 0, 0, tiled=True).reshape(nrows, row_block)
    fit_other = other_core(fit_own)

    mine = lax.dynamic_slice_in_dim(points, plane_index * row_block, row_block, 0)
    theirs_index = plane_index + (1 - 2 * core) * lax.axis_size("pts")
    theirs = lax.dynamic_slice_in_dim(points, theirs_index * row_block, row_block, 0)
    block = lax.dynamic_slice_in_dim(points, grid_index * column_block, column_block, 0)
    wanted = jnp.concatenate([mine, theirs, block])
    half_of = lax.rem(wanted, rows_dev) // part
    spots = (half_of ^ pts) * (nrows // 2) + wanted // rows_dev * part + lax.rem(wanted, part)
    density, density_other, picked, columns = pick(spots, pieces, row_block)

    density = density + other_core(density_other)
    masked = (density * screened.astype(F32)).astype(BF)
    masked, fit_own = lax.optimization_barrier((masked, fit_own))
    masked_other = other_core(masked)

    applied = summed_on_grid(
        applied_shares(grid_index[None], picked, masked, masked_other, n_grid, share)
    )
    applied = applied.reshape(4, 2, 2 * share, 2 * row_block)
    applied = jnp.where(xh == 0, applied, applied[:, ::-1])
    applied = lax.dynamic_slice_in_dim(
        jnp.concatenate([applied, applied]), lax.rem(4 - y, 4), 4, 0
    ).reshape(-1, 2 * row_block)
    terms = sum(
        lax.dot_general(a, f, (((1,), (1,)), ((), ())), preferred_element_type=F32)
        for a, f in ((applied[:, :row_block], fit_own), (applied[:, row_block:], fit_other))
    ).astype(BF)
    parts = lax.all_to_all(terms.reshape(-1, share, nrows), CHIPS, 0, 0, tiled=True)
    exchange = -jnp.sum(parts.astype(F32), axis=0)
    exchange = jnp.stack([exchange, other_core(exchange)])
    exchange = jnp.where(core == 0, exchange, exchange[::-1])

    halves = exchange.astype(BF).reshape(2 * share, n_grid, 2, part)
    halves = jnp.where(pts == 0, halves, halves[:, :, ::-1])
    halves = halves.transpose(0, 2, 1, 3).reshape(2 * share, nrows)
    matrix = lax.dot_general(
        halves, columns, (((1,), (1,)), ((), ())), preferred_element_type=F32
    ) / math.sqrt(nrows)
    matrix = matrix.transpose(1, 0, 2).reshape(4, 2 * share, 2, width).transpose(0, 2, 1, 3)
    matrix = jnp.where(xh == 0, matrix, matrix[:, ::-1])
    matrix = lax.dynamic_slice_in_dim(
        jnp.concatenate([matrix, matrix]), lax.rem(4 - y, 4), 4, 0
    ).reshape(n_grid, 2, share, width)
    mine = exchange.reshape(2, share, n_grid, 2, width)
    mine = lax.dynamic_index_in_dim(mine, core, 3, keepdims=False).transpose(2, 0, 1, 3)
    both = jnp.stack([mine, matrix], axis=2).reshape(2 * n_grid, 2, share, width)
    both = lax.all_to_all(both, ("grid", "core"), 0, 0, tiled=True)
    both = both.reshape(n_grid, 2, 2, share, width).transpose(2, 0, 3, 1, 4)
    both = both.reshape(2, n_grid * share, 2 * width)
    return both[0], both[1]


def solution(mesh):
    n_grid, n_orb, n_pts = (mesh.shape[a] for a in ("grid", "orb", "pts"))
    fine = Mesh(
        mesh.devices.reshape(n_grid, n_orb // 4, 2, 2, n_pts),
        ("grid", "y", "xh", "core", "pts"),
    )
    in_specs = (P("grid", ORB), P(), P("grid", PLANE), P(PLANE, "grid"))
    out_specs = (P(PLANE, "grid"), P(PLANE, "grid"))
    return jax.shard_map(body, mesh=fine, in_specs=in_specs, out_specs=out_specs, check_vma=False)
```

```python
import math

import jax
import jax.numpy as jnp
from jax import lax
from jax.experimental import pallas as pl
from jax.experimental.pallas import tpu as pltpu
from jax.sharding import Mesh, PartitionSpec as P


BF = jnp.bfloat16
F32 = jnp.float32
ORB = ("y", "xh", "core")
PLANE = ("y", "xh", "core", "pts")
CHIPS = ("y", "xh", "pts")
X = ("xh", "pts")


def sent_to_all(x, axis):
    copies = jnp.broadcast_to(x, (lax.axis_size(axis), *x.shape))
    return lax.all_to_all(copies, axis, split_axis=0, concat_axis=0, tiled=True)


def from_next(x, step):
    n = lax.axis_size("y")
    return lax.ppermute(x, "y", [(i, (i - step) % n) for i in range(n)])


def with_twin(x):
    return lax.ppermute(x, X, [(0, 1), (1, 0), (2, 3), (3, 2)])


def with_mirror(x):
    return lax.ppermute(x, X, [(0, 3), (3, 0), (1, 2), (2, 1)])


def with_far(x):
    return lax.ppermute(x, X, [(0, 2), (2, 0), (1, 3), (3, 1)])


def along_y(first, second):
    after, before = from_next(first, 1), from_next(first, -1)
    after2, before2 = from_next(second, 1), from_next(second, -1)
    far = from_next(after, 1)
    far2 = from_next(before2, -1)
    return (first, after, far, before), (second, after2, far2, before2)


def along_x(first, second):
    twin, mirror = with_twin(first), with_mirror(first)
    twin2, mirror2 = with_twin(second), with_mirror(second)
    far = with_twin(mirror)
    far2 = with_mirror(twin2)
    return (first, twin, mirror, far), (second, twin2, mirror2, far2)


def other_core(x):
    return lax.ppermute(x, "core", [(0, 1), (1, 0)])


def pick_kernel(spots_ref, place_ref, *refs):
    pieces, (own_ref, other_ref, picked_out_ref, columns_out_ref) = refs[:16], refs[16:20]
    wide_ref, chosen_ref, rows_ref, picked_ref, columns_ref, sems = refs[20:]
    rows = own_ref.shape[0]
    rest = picked_ref.shape[0]
    height, width = pieces[0].shape[1:]
    alpha, beta = pieces[:8], pieces[8:]
    pts, y, xh = (place_ref[k] for k in range(3))
    part = height // 4
    group = 256

    for at in range(4):
        for col, roles in enumerate(((0, 1), (3, 2))):
            spot = 2 * lax.rem(y + at, 4) + (xh if col == 0 else 1 - xh)
            for k, role in enumerate(roles):
                half = pts if k == 0 else 1 - pts
                for low, (piece, which) in enumerate(
                    ((alpha[role + 4 * (at // 2)], at % 2), (beta[at + 4 * (role // 2)], role % 2))
                ):

                    def spread(i, _, piece=piece, which=which, low=low, spot=spot, half=half):
                        block = piece[which, pl.ds(pl.multiple_of(i * part, part), part), :]
                        row = pl.multiple_of((4 * low + i) * 2 * part + half * part, part)
                        columns_ref[spot, pl.ds(row, part), :] = block
                        wide_ref[pl.ds(row * 8 + spot, part, stride=8), :] = block.astype(F32)
                        return _

                    lax.fori_loop(0, 4, spread, 0)

    keep_columns = pltpu.make_async_copy(columns_ref, columns_out_ref, sems.at[0])
    keep_columns.start()

    def choose(i, _):
        for k in range(16):
            spot = pl.multiple_of(spots_ref[i * 16 + k] * 8, 8)
            to = pl.multiple_of(i * 128 + k * 8, 8)
            chosen_ref[pl.ds(to, 8), :] = wide_ref[pl.ds(spot, 8), :]
        return _

    lax.fori_loop(0, (2 * rows + rest) // 16, choose, 0)

    for target, first, count in ((picked_ref, 2 * rows, rest), (rows_ref, 0, 2 * rows)):
        for k in range(8):

            def gather(i, _, target=target, first=first, k=k):
                start = pl.multiple_of(i * group, group)
                block = chosen_ref[pl.ds((first + start) * 8 + k, group, stride=8), :]
                target[pl.ds(start, group), k * width : (k + 1) * width] = block.astype(BF)
                return _

            lax.fori_loop(0, count // group, gather, 0)

    keep_picked = pltpu.make_async_copy(picked_ref, picked_out_ref, sems.at[1])
    keep_picked.start()
    for k, out in enumerate((own_ref, other_ref)):
        out[...] = lax.dot_general(
            rows_ref[k * rows : (k + 1) * rows],
            picked_ref[...],
            (((1,), (1,)), ((), ())),
            preferred_element_type=F32,
        )
    keep_columns.wait()
    keep_picked.wait()


def pick(spots, place, pieces, rows):
    _, height, width = pieces[0].shape
    total, nrows = spots.shape[0], 4 * height
    rest = total - 2 * rows
    vm = pl.BlockSpec(memory_space=pltpu.VMEM)
    sm = pl.BlockSpec(memory_space=pltpu.SMEM)
    hbm = pl.BlockSpec(memory_space=pltpu.HBM)
    return pl.pallas_call(
        pick_kernel,
        in_specs=[sm, sm] + [vm] * 16,
        out_specs=[vm, vm, hbm, hbm],
        out_shape=[
            jax.ShapeDtypeStruct((rows, rest), F32),
            jax.ShapeDtypeStruct((rows, rest), F32),
            pltpu.HBM((rest, 8 * width), BF),
            pltpu.HBM((8, nrows, width), BF),
        ],
        scratch_shapes=[
            pltpu.VMEM((nrows * 8, width), F32),
            pltpu.VMEM((total * 8, width), F32),
            pltpu.VMEM((2 * rows, 8 * width), BF),
            pltpu.VMEM((rest, 8 * width), BF),
            pltpu.VMEM((8, nrows, width), BF),
            pltpu.SemaphoreType.DMA((2,)),
        ],
        compiler_params=pltpu.CompilerParams(vmem_limit_bytes=28 << 20),
        cost_estimate=pl.CostEstimate(
            flops=4 * rows * rest * 8 * width, bytes_accessed=32 * nrows * width, transcendentals=0
        ),
        name="pick",
    )(spots, place, *pieces)


def apply_kernel(place_ref, picked_ref, own_ref, other_ref, *refs):
    outs, held_ref = refs[:-1], refs[-1]
    rows = own_ref.shape[0]
    groups, n, share, _ = held_ref.shape
    for k, ref in enumerate((own_ref, other_ref)):
        product = jnp.dot(ref[...], picked_ref[...], preferred_element_type=F32)
        held_ref[:, :, :, k * rows : (k + 1) * rows] = product.T.reshape(groups, n, share, rows)
    for k, out in enumerate(outs[:n]):
        if k == n // 2:
            half = groups // 2
            spot = lax.rem(place_ref[0] + k, n)
            out[...] = held_ref[:half, spot].astype(BF)
            outs[n][...] = held_ref[half:, spot].astype(BF)
        else:
            out[...] = held_ref[:, lax.rem(place_ref[0] + k, n)].astype(BF)


def applied_shares(place, picked, own, other, n, share):
    rows, columns = own.shape[0], picked.shape[1]
    groups = columns // (n * share)
    vm = pl.BlockSpec(memory_space=pltpu.VMEM)
    counts = [groups] * n + [groups // 2]
    counts[n // 2] = groups // 2
    return pl.pallas_call(
        apply_kernel,
        in_specs=[pl.BlockSpec(memory_space=pltpu.SMEM)] + [vm] * 3,
        out_specs=[vm] * (n + 1),
        out_shape=[jax.ShapeDtypeStruct((c, share, 2 * rows), BF) for c in counts],
        scratch_shapes=[pltpu.VMEM((groups, n, share, 2 * rows), F32)],
        compiler_params=pltpu.CompilerParams(vmem_limit_bytes=16 << 20),
        cost_estimate=pl.CostEstimate(
            flops=4 * rows * columns * own.shape[1], bytes_accessed=8 * rows * columns, transcendentals=0
        ),
        name="applied",
    )(place, picked, own, other)


def to_grid(x, step):
    n = lax.axis_size("grid")
    return lax.ppermute(x, "grid", [(i, (i + step) % n) for i in range(n)])


def summed_on_grid(shares):
    total = shares[0].astype(F32)
    opposite = {1: shares[4], -1: shares[8]}
    near = {1: shares[1], -1: shares[7]}
    second = {1: shares[2], -1: shares[6]}
    third = {1: shares[3], -1: shares[5]}
    opposite = {way: to_grid(x, 3 * way) for way, x in opposite.items()}
    third = {way: to_grid(x, 2 * way) for way, x in third.items()}
    second = {way: to_grid(x, way) for way, x in second.items()}
    sums = []
    for way in (1, -1):
        none = jnp.zeros_like(opposite[way])
        both = [opposite[way], none] if way == 1 else [none, opposite[way]]
        terms = near[way], second[way], third[way], jnp.concatenate(both)
        sums.append(to_grid(sum(t.astype(F32) for t in terms).astype(BF), way))
    return (total + sums[0].astype(F32) + sums[1].astype(F32)).astype(BF)


def body(orbitals, points, fitting, screened):
    n_grid = lax.axis_size("grid")
    n_plane = lax.axis_size(PLANE)
    grid_index = lax.axis_index("grid")
    plane_index = lax.axis_index(PLANE)
    y, xh, core, pts = (lax.axis_index(a) for a in PLANE)
    rows_dev, width = orbitals.shape
    nrows = rows_dev * n_grid
    nfull = width * lax.axis_size(ORB)
    npoints = points.shape[0]
    row_block = npoints // n_plane
    column_block = npoints // n_grid
    share = nfull // (n_plane * n_grid)
    part = rows_dev // 2
    quarter = nrows // 4

    own_rows = lax.dynamic_slice_in_dim(orbitals, pts * part, part, 0)
    held = sent_to_all(own_rows, "grid").reshape(2, quarter, width)
    alpha, beta = held[0], held[1]
    alphas = [alpha, from_next(alpha, 1), from_next(alpha, 2), from_next(alpha, -1)]
    betas = [beta, with_twin(beta), with_mirror(beta), with_far(beta)]
    a_first, a_second = jnp.stack(alphas[:2]), jnp.stack(alphas[2:])
    b_first, b_second = jnp.stack(betas[:2]), jnp.stack(betas[2:])
    pieces = [x for part in along_x(a_first, a_second) + along_y(b_first, b_second) for x in part]

    copies = jnp.broadcast_to(fitting, (n_grid, *fitting.shape))
    fit_own = lax.all_to_all(copies, "grid", 0, 0, tiled=True).reshape(nrows, row_block)
    fit_other = other_core(fit_own)

    mine = lax.dynamic_slice_in_dim(points, plane_index * row_block, row_block, 0)
    theirs_index = plane_index + (1 - 2 * core) * lax.axis_size("pts")
    theirs = lax.dynamic_slice_in_dim(points, theirs_index * row_block, row_block, 0)
    block = lax.dynamic_slice_in_dim(points, grid_index * column_block, column_block, 0)
    wanted = jnp.concatenate([mine, theirs, block])
    place = jnp.stack([pts, y, xh])
    density, density_other, picked, columns = pick(wanted, place, pieces, row_block)

    density = density + other_core(density_other)
    masked = (density * screened.astype(F32)).astype(BF)
    masked_other = other_core(masked)
    masked_other, fit_own = lax.optimization_barrier((masked_other, fit_own))

    applied = summed_on_grid(
        applied_shares(grid_index[None], picked, masked, masked_other, n_grid, share)
    )
    applied = applied.reshape(-1, 2 * row_block)
    terms = sum(
        lax.dot_general(a, f, (((1,), (1,)), ((), ())), preferred_element_type=F32)
        for a, f in ((applied[:, :row_block], fit_own), (applied[:, row_block:], fit_other))
    ).astype(BF)
    parts = lax.all_to_all(terms.reshape(-1, share, nrows), CHIPS, 0, 0, tiled=True)
    exchange = -jnp.sum(parts.astype(F32), axis=0)
    exchange = jnp.stack([exchange, other_core(exchange)])
    exchange = jnp.where(core == 0, exchange, exchange[::-1])

    rounded = exchange.astype(BF).reshape(2 * share, nrows)
    matrix = lax.dot_general(
        rounded, columns, (((1,), (1,)), ((), ())), preferred_element_type=F32
    ) / math.sqrt(nrows)
    matrix = matrix.reshape(2, share, n_grid, width).transpose(2, 0, 1, 3)
    mine = exchange.reshape(2, share, n_grid, 2, width)
    mine = lax.dynamic_index_in_dim(mine, core, 3, keepdims=False).transpose(2, 0, 1, 3)
    both = jnp.stack([mine, matrix], axis=2).reshape(2 * n_grid, 2, share, width)
    both = lax.all_to_all(both, ("grid", "core"), 0, 0, tiled=True)
    both = both.reshape(n_grid, 2, 2, share, width).transpose(2, 0, 3, 1, 4)
    both = both.reshape(2, n_grid * share, 2 * width)
    return both[0], both[1]


def solution(mesh):
    n_grid, n_orb, n_pts = (mesh.shape[a] for a in ("grid", "orb", "pts"))
    fine = Mesh(
        mesh.devices.reshape(n_grid, n_orb // 4, 2, 2, n_pts),
        ("grid", "y", "xh", "core", "pts"),
    )
    in_specs = (P("grid", ORB), P(), P("grid", PLANE), P(PLANE, "grid"))
    out_specs = (P(PLANE, "grid"), P(PLANE, "grid"))
    return jax.shard_map(body, mesh=fine, in_specs=in_specs, out_specs=out_specs, check_vma=False)
```

```python
import math

import jax
import jax.numpy as jnp
from jax import lax
from jax.experimental import pallas as pl
from jax.experimental.pallas import tpu as pltpu
from jax.sharding import Mesh, PartitionSpec as P


BF = jnp.bfloat16
F32 = jnp.float32
ORB = ("y", "xh", "core")
PLANE = ("y", "xh", "core", "pts")
CHIPS = ("y", "xh", "pts")
X = ("xh", "pts")


def sent_to_all(x, axis):
    copies = jnp.broadcast_to(x, (lax.axis_size(axis), *x.shape))
    return lax.all_to_all(copies, axis, split_axis=0, concat_axis=0, tiled=True)


def from_next(x, step):
    n = lax.axis_size("y")
    return lax.ppermute(x, "y", [(i, (i - step) % n) for i in range(n)])


def with_twin(x):
    return lax.ppermute(x, X, [(0, 1), (1, 0), (2, 3), (3, 2)])


def with_mirror(x):
    return lax.ppermute(x, X, [(0, 3), (3, 0), (1, 2), (2, 1)])


def with_far(x):
    return lax.ppermute(x, X, [(0, 2), (2, 0), (1, 3), (3, 1)])


def along_y(first, second):
    after, before = from_next(first, 1), from_next(first, -1)
    after2, before2 = from_next(second, 1), from_next(second, -1)
    far = from_next(after, 1)
    far2 = from_next(before2, -1)
    return (first, after, far, before), (second, after2, far2, before2)


def along_x(first, second):
    twin, mirror = with_twin(first), with_mirror(first)
    twin2, mirror2 = with_twin(second), with_mirror(second)
    far = with_twin(mirror)
    far2 = with_mirror(twin2)
    return (first, twin, mirror, far), (second, twin2, mirror2, far2)


def other_core(x):
    return lax.ppermute(x, "core", [(0, 1), (1, 0)])


def pick_kernel(spots_ref, place_ref, *refs):
    pieces, (own_ref, other_ref, picked_out_ref, columns_out_ref) = refs[:16], refs[16:20]
    wide_ref, chosen_ref, rows_ref, picked_ref, columns_ref, sems = refs[20:]
    rows = own_ref.shape[0]
    rest = picked_ref.shape[0]
    height, width = pieces[0].shape[1:]
    alpha, beta = pieces[:8], pieces[8:]
    pts, y, xh = (place_ref[k] for k in range(3))
    part = height // 4
    group = 256

    for at in range(4):
        for col, roles in enumerate(((0, 1), (3, 2))):
            spot = 2 * lax.rem(y + at, 4) + (xh if col == 0 else 1 - xh)
            for k, role in enumerate(roles):
                half = pts if k == 0 else 1 - pts
                for low, (piece, which) in enumerate(
                    ((alpha[role + 4 * (at // 2)], at % 2), (beta[at + 4 * (role // 2)], role % 2))
                ):

                    def spread(i, _, piece=piece, which=which, low=low, spot=spot, half=half):
                        block = piece[which, pl.ds(pl.multiple_of(i * part, part), part), :]
                        row = pl.multiple_of((4 * low + i) * 2 * part + half * part, part)
                        columns_ref[spot, pl.ds(row, part), :] = block
                        wide_ref[pl.ds(row * 8 + spot, part, stride=8), :] = block.astype(F32)
                        return _

                    lax.fori_loop(0, 4, spread, 0)

    keep_columns = pltpu.make_async_copy(columns_ref, columns_out_ref, sems.at[0])
    keep_columns.start()

    def choose(i, _):
        for k in range(16):
            spot = pl.multiple_of(spots_ref[i * 16 + k] * 8, 8)
            to = pl.multiple_of(i * 128 + k * 8, 8)
            chosen_ref[pl.ds(to, 8), :] = wide_ref[pl.ds(spot, 8), :]
        return _

    lax.fori_loop(0, (2 * rows + rest) // 16, choose, 0)

    for target, first, count in ((picked_ref, 2 * rows, rest), (rows_ref, 0, 2 * rows)):
        for k in range(8):

            def gather(i, _, target=target, first=first, k=k):
                start = pl.multiple_of(i * group, group)
                block = chosen_ref[pl.ds((first + start) * 8 + k, group, stride=8), :]
                target[pl.ds(start, group), k * width : (k + 1) * width] = block.astype(BF)
                return _

            lax.fori_loop(0, count // group, gather, 0)

    keep_picked = pltpu.make_async_copy(picked_ref, picked_out_ref, sems.at[1])
    keep_picked.start()
    for k, out in enumerate((own_ref, other_ref)):
        out[...] = lax.dot_general(
            rows_ref[k * rows : (k + 1) * rows],
            picked_ref[...],
            (((1,), (1,)), ((), ())),
            preferred_element_type=F32,
        )
    keep_columns.wait()
    keep_picked.wait()


def pick(spots, place, pieces, rows):
    _, height, width = pieces[0].shape
    total, nrows = spots.shape[0], 4 * height
    rest = total - 2 * rows
    vm = pl.BlockSpec(memory_space=pltpu.VMEM)
    sm = pl.BlockSpec(memory_space=pltpu.SMEM)
    hbm = pl.BlockSpec(memory_space=pltpu.HBM)
    return pl.pallas_call(
        pick_kernel,
        in_specs=[sm, sm] + [vm] * 16,
        out_specs=[vm, vm, hbm, hbm],
        out_shape=[
            jax.ShapeDtypeStruct((rows, rest), F32),
            jax.ShapeDtypeStruct((rows, rest), F32),
            pltpu.HBM((rest, 8 * width), BF),
            pltpu.HBM((8, nrows, width), BF),
        ],
        scratch_shapes=[
            pltpu.VMEM((nrows * 8, width), F32),
            pltpu.VMEM((total * 8, width), F32),
            pltpu.VMEM((2 * rows, 8 * width), BF),
            pltpu.VMEM((rest, 8 * width), BF),
            pltpu.VMEM((8, nrows, width), BF),
            pltpu.SemaphoreType.DMA((2,)),
        ],
        compiler_params=pltpu.CompilerParams(vmem_limit_bytes=28 << 20),
        cost_estimate=pl.CostEstimate(
            flops=4 * rows * rest * 8 * width, bytes_accessed=32 * nrows * width, transcendentals=0
        ),
        name="pick",
    )(spots, place, *pieces)


def product_kernel(picked_ref, rows_ref, out_ref):
    product = jnp.dot(rows_ref[...], picked_ref[...], preferred_element_type=F32)
    out_ref[...] = product.T.reshape(out_ref.shape).astype(BF)


def applied_rows(picked, rows, n, share):
    count, columns = rows.shape[0], picked.shape[1]
    vm = pl.BlockSpec(memory_space=pltpu.VMEM)
    return pl.pallas_call(
        product_kernel,
        in_specs=[vm] * 2,
        out_specs=vm,
        out_shape=jax.ShapeDtypeStruct((columns // (n * share), n, share, count), BF),
        compiler_params=pltpu.CompilerParams(vmem_limit_bytes=16 << 20),
        cost_estimate=pl.CostEstimate(
            flops=2 * count * columns * rows.shape[1], bytes_accessed=4 * count * columns, transcendentals=0
        ),
        name="own",
    )(picked, rows)


def apply_kernel(place_ref, picked_ref, own_ref, other_ref, *refs):
    outs, held_ref = refs[:-1], refs[-1]
    rows = other_ref.shape[0]
    groups, n, _, _ = held_ref.shape
    half = groups // 2
    product = jnp.dot(other_ref[...], picked_ref[...], preferred_element_type=F32)
    held_ref[...] = product.T.reshape(held_ref.shape)
    for k, out in enumerate(outs[:n]):
        spot = lax.rem(place_ref[0] + k, n)
        split = [(out, 0, groups)] if k != n // 2 else [(out, 0, half), (outs[n], half, groups)]
        for target, low, high in split:
            target[:, :, :rows] = own_ref[low:high, spot]
            target[:, :, rows:] = held_ref[low:high, spot].astype(BF)


def applied_shares(place, picked, own, other):
    groups, n, share, rows = own.shape
    columns = picked.shape[1]
    vm = pl.BlockSpec(memory_space=pltpu.VMEM)
    counts = [groups] * n + [groups // 2]
    counts[n // 2] = groups // 2
    return pl.pallas_call(
        apply_kernel,
        in_specs=[pl.BlockSpec(memory_space=pltpu.SMEM)] + [vm] * 3,
        out_specs=[vm] * (n + 1),
        out_shape=[jax.ShapeDtypeStruct((c, share, 2 * rows), BF) for c in counts],
        scratch_shapes=[pltpu.VMEM((groups, n, share, rows), F32)],
        compiler_params=pltpu.CompilerParams(vmem_limit_bytes=16 << 20),
        cost_estimate=pl.CostEstimate(
            flops=2 * rows * columns * other.shape[1], bytes_accessed=8 * rows * columns, transcendentals=0
        ),
        name="applied",
    )(place, picked, own, other)


def to_grid(x, step):
    n = lax.axis_size("grid")
    return lax.ppermute(x, "grid", [(i, (i + step) % n) for i in range(n)])


def summed_on_grid(shares):
    total = shares[0].astype(F32)
    opposite = {1: shares[4], -1: shares[8]}
    near = {1: shares[1], -1: shares[7]}
    second = {1: shares[2], -1: shares[6]}
    third = {1: shares[3], -1: shares[5]}
    opposite = {way: to_grid(x, 3 * way) for way, x in opposite.items()}
    third = {way: to_grid(x, 2 * way) for way, x in third.items()}
    second = {way: to_grid(x, way) for way, x in second.items()}
    sums = []
    for way in (1, -1):
        none = jnp.zeros_like(opposite[way])
        both = [opposite[way], none] if way == 1 else [none, opposite[way]]
        terms = near[way], second[way], third[way], jnp.concatenate(both)
        sums.append(to_grid(sum(t.astype(F32) for t in terms).astype(BF), way))
    return (total + sums[0].astype(F32) + sums[1].astype(F32)).astype(BF)


def body(orbitals, points, fitting, screened):
    n_grid = lax.axis_size("grid")
    n_plane = lax.axis_size(PLANE)
    grid_index = lax.axis_index("grid")
    plane_index = lax.axis_index(PLANE)
    y, xh, core, pts = (lax.axis_index(a) for a in PLANE)
    rows_dev, width = orbitals.shape
    nrows = rows_dev * n_grid
    nfull = width * lax.axis_size(ORB)
    npoints = points.shape[0]
    row_block = npoints // n_plane
    column_block = npoints // n_grid
    share = nfull // (n_plane * n_grid)
    part = rows_dev // 2
    quarter = nrows // 4

    own_rows = lax.dynamic_slice_in_dim(orbitals, pts * part, part, 0)
    held = sent_to_all(own_rows, "grid").reshape(2, quarter, width)
    alpha, beta = held[0], held[1]
    alphas = [alpha, from_next(alpha, 1), from_next(alpha, 2), from_next(alpha, -1)]
    betas = [beta, with_twin(beta), with_mirror(beta), with_far(beta)]
    a_first, a_second = jnp.stack(alphas[:2]), jnp.stack(alphas[2:])
    b_first, b_second = jnp.stack(betas[:2]), jnp.stack(betas[2:])
    pieces = [x for part in along_x(a_first, a_second) + along_y(b_first, b_second) for x in part]

    copies = jnp.broadcast_to(fitting, (n_grid, *fitting.shape))
    fit_own = lax.all_to_all(copies, "grid", 0, 0, tiled=True).reshape(nrows, row_block)
    fit_other = other_core(fit_own)

    mine = lax.dynamic_slice_in_dim(points, plane_index * row_block, row_block, 0)
    theirs_index = plane_index + (1 - 2 * core) * lax.axis_size("pts")
    theirs = lax.dynamic_slice_in_dim(points, theirs_index * row_block, row_block, 0)
    block = lax.dynamic_slice_in_dim(points, grid_index * column_block, column_block, 0)
    wanted = jnp.concatenate([mine, theirs, block])
    place = jnp.stack([pts, y, xh])
    density, density_other, picked, columns = pick(wanted, place, pieces, row_block)

    density = density + other_core(density_other)
    masked = (density * screened.astype(F32)).astype(BF)
    masked_other = other_core(masked)
    applied_own = applied_rows(picked, masked, n_grid, share)
    masked_other, fit_own = lax.optimization_barrier((masked_other, fit_own))

    applied = summed_on_grid(
        applied_shares(grid_index[None], picked, applied_own, masked_other)
    )
    applied = applied.reshape(-1, 2 * row_block)
    terms = sum(
        lax.dot_general(a, f, (((1,), (1,)), ((), ())), preferred_element_type=F32)
        for a, f in ((applied[:, :row_block], fit_own), (applied[:, row_block:], fit_other))
    ).astype(BF)
    parts = lax.all_to_all(terms.reshape(-1, share, nrows), CHIPS, 0, 0, tiled=True)
    exchange = -jnp.sum(parts.astype(F32), axis=0)
    exchange = jnp.stack([exchange, other_core(exchange)])
    exchange = jnp.where(core == 0, exchange, exchange[::-1])

    rounded = exchange.astype(BF).reshape(2 * share, nrows)
    matrix = lax.dot_general(
        rounded, columns, (((1,), (1,)), ((), ())), preferred_element_type=F32
    ) / math.sqrt(nrows)
    matrix = matrix.reshape(2, share, n_grid, width).transpose(2, 0, 1, 3)
    mine = exchange.reshape(2, share, n_grid, 2, width)
    mine = lax.dynamic_index_in_dim(mine, core, 3, keepdims=False).transpose(2, 0, 1, 3)
    both = jnp.stack([mine, matrix], axis=2).reshape(2 * n_grid, 2, share, width)
    both = lax.all_to_all(both, ("grid", "core"), 0, 0, tiled=True)
    both = both.reshape(n_grid, 2, 2, share, width).transpose(2, 0, 3, 1, 4)
    both = both.reshape(2, n_grid * share, 2 * width)
    return both[0], both[1]


def solution(mesh):
    n_grid, n_orb, n_pts = (mesh.shape[a] for a in ("grid", "orb", "pts"))
    fine = Mesh(
        mesh.devices.reshape(n_grid, n_orb // 4, 2, 2, n_pts),
        ("grid", "y", "xh", "core", "pts"),
    )
    in_specs = (P("grid", ORB), P(), P("grid", PLANE), P(PLANE, "grid"))
    out_specs = (P(PLANE, "grid"), P(PLANE, "grid"))
    return jax.shard_map(body, mesh=fine, in_specs=in_specs, out_specs=out_specs, check_vma=False)
```

```python
import math

import jax
import jax.numpy as jnp
from jax import lax
from jax.experimental import pallas as pl
from jax.experimental.pallas import tpu as pltpu
from jax.sharding import Mesh, PartitionSpec as P


BF = jnp.bfloat16
F32 = jnp.float32
ORB = ("y", "xh", "core")
PLANE = ("y", "xh", "core", "pts")
CHIPS = ("y", "xh", "pts")
X = ("xh", "pts")


def sent_to_all(x, axis):
    copies = jnp.broadcast_to(x, (lax.axis_size(axis), *x.shape))
    return lax.all_to_all(copies, axis, split_axis=0, concat_axis=0, tiled=True)


def from_next(x, step):
    n = lax.axis_size("y")
    return lax.ppermute(x, "y", [(i, (i - step) % n) for i in range(n)])


def with_twin(x):
    return lax.ppermute(x, X, [(0, 1), (1, 0), (2, 3), (3, 2)])


def with_mirror(x):
    return lax.ppermute(x, X, [(0, 3), (3, 0), (1, 2), (2, 1)])


def with_far(x):
    return lax.ppermute(x, X, [(0, 2), (2, 0), (1, 3), (3, 1)])


def along_y(first, second):
    after, before = from_next(first, 1), from_next(first, -1)
    after2, before2 = from_next(second, 1), from_next(second, -1)
    far = from_next(after, 1)
    far2 = from_next(before2, -1)
    return (first, after, far, before), (second, after2, far2, before2)


def along_x(first, second):
    twin, mirror = with_twin(first), with_mirror(first)
    twin2, mirror2 = with_twin(second), with_mirror(second)
    far = with_twin(mirror)
    far2 = with_mirror(twin2)
    return (first, twin, mirror, far), (second, twin2, mirror2, far2)


def other_core(x):
    return lax.ppermute(x, "core", [(0, 1), (1, 0)])


def pick_kernel(spots_ref, place_ref, *refs):
    pieces, (own_ref, other_ref, picked_out_ref, columns_out_ref) = refs[:16], refs[16:20]
    wide_ref, chosen_ref, rows_ref, picked_ref, columns_ref, sems = refs[20:]
    rows = own_ref.shape[0]
    rest = picked_ref.shape[0]
    height, width = pieces[0].shape[1:]
    alpha, beta = pieces[:8], pieces[8:]
    pts, y, xh = (place_ref[k] for k in range(3))
    part = height // 4
    group = 512

    for at in range(4):
        for col, roles in enumerate(((0, 1), (3, 2))):
            spot = 2 * lax.rem(y + at, 4) + (xh if col == 0 else 1 - xh)
            for k, role in enumerate(roles):
                half = pts if k == 0 else 1 - pts
                for low, (piece, which) in enumerate(
                    ((alpha[role + 4 * (at // 2)], at % 2), (beta[at + 4 * (role // 2)], role % 2))
                ):

                    def spread(i, _, piece=piece, which=which, low=low, spot=spot, half=half):
                        for step in (2 * i, 2 * i + 1):
                            block = piece[which, pl.ds(pl.multiple_of(step * part, part), part), :]
                            row = pl.multiple_of((4 * low + step) * 2 * part + half * part, part)
                            columns_ref[spot, pl.ds(row, part), :] = block
                            wide_ref[pl.ds(row * 8 + spot, part, stride=8), :] = block.astype(F32)
                        return _

                    lax.fori_loop(0, 2, spread, 0)

    keep_columns = pltpu.make_async_copy(columns_ref, columns_out_ref, sems.at[0])
    keep_columns.start()

    def choose(i, _):
        for k in range(32):
            spot = pl.multiple_of(spots_ref[i * 32 + k] * 8, 8)
            to = pl.multiple_of(i * 256 + k * 8, 8)
            chosen_ref[pl.ds(to, 8), :] = wide_ref[pl.ds(spot, 8), :]
        return _

    lax.fori_loop(0, (2 * rows + rest) // 32, choose, 0)

    for target, first, count in ((picked_ref, 2 * rows, rest), (rows_ref, 0, 2 * rows)):
        for k in range(8):

            def gather(i, _, target=target, first=first, k=k):
                start = pl.multiple_of(i * group, group)
                block = chosen_ref[pl.ds((first + start) * 8 + k, group, stride=8), :]
                target[pl.ds(start, group), k * width : (k + 1) * width] = block.astype(BF)
                return _

            lax.fori_loop(0, count // group, gather, 0)

    keep_picked = pltpu.make_async_copy(picked_ref, picked_out_ref, sems.at[1])
    keep_picked.start()
    for k, out in enumerate((own_ref, other_ref)):
        out[...] = lax.dot_general(
            rows_ref[k * rows : (k + 1) * rows],
            picked_ref[...],
            (((1,), (1,)), ((), ())),
            preferred_element_type=F32,
        )
    keep_columns.wait()
    keep_picked.wait()


def pick(spots, place, pieces, rows):
    _, height, width = pieces[0].shape
    total, nrows = spots.shape[0], 4 * height
    rest = total - 2 * rows
    vm = pl.BlockSpec(memory_space=pltpu.VMEM)
    sm = pl.BlockSpec(memory_space=pltpu.SMEM)
    hbm = pl.BlockSpec(memory_space=pltpu.HBM)
    return pl.pallas_call(
        pick_kernel,
        in_specs=[sm, sm] + [vm] * 16,
        out_specs=[vm, vm, hbm, hbm],
        out_shape=[
            jax.ShapeDtypeStruct((rows, rest), F32),
            jax.ShapeDtypeStruct((rows, rest), F32),
            pltpu.HBM((rest, 8 * width), BF),
            pltpu.HBM((8, nrows, width), BF),
        ],
        scratch_shapes=[
            pltpu.VMEM((nrows * 8, width), F32),
            pltpu.VMEM((total * 8, width), F32),
            pltpu.VMEM((2 * rows, 8 * width), BF),
            pltpu.VMEM((rest, 8 * width), BF),
            pltpu.VMEM((8, nrows, width), BF),
            pltpu.SemaphoreType.DMA((2,)),
        ],
        compiler_params=pltpu.CompilerParams(vmem_limit_bytes=28 << 20),
        cost_estimate=pl.CostEstimate(
            flops=4 * rows * rest * 8 * width, bytes_accessed=32 * nrows * width, transcendentals=0
        ),
        name="pick",
    )(spots, place, *pieces)


def product_kernel(picked_ref, rows_ref, out_ref):
    product = jnp.dot(rows_ref[...], picked_ref[...], preferred_element_type=F32)
    out_ref[...] = product.T.reshape(out_ref.shape).astype(BF)


def applied_rows(picked, rows, n, share):
    count, columns = rows.shape[0], picked.shape[1]
    vm = pl.BlockSpec(memory_space=pltpu.VMEM)
    return pl.pallas_call(
        product_kernel,
        in_specs=[vm] * 2,
        out_specs=vm,
        out_shape=jax.ShapeDtypeStruct((columns // (n * share), n, share, count), BF),
        compiler_params=pltpu.CompilerParams(vmem_limit_bytes=16 << 20),
        cost_estimate=pl.CostEstimate(
            flops=2 * count * columns * rows.shape[1], bytes_accessed=4 * count * columns, transcendentals=0
        ),
        name="own",
    )(picked, rows)


def apply_kernel(place_ref, picked_ref, own_ref, other_ref, *refs):
    outs, held_ref = refs[:-1], refs[-1]
    rows = other_ref.shape[0]
    groups, n, _, _ = held_ref.shape
    half = groups // 2
    product = jnp.dot(other_ref[...], picked_ref[...], preferred_element_type=F32)
    held_ref[...] = product.T.reshape(held_ref.shape)
    for k, out in enumerate(outs[:n]):
        spot = lax.rem(place_ref[0] + k, n)
        split = [(out, 0, groups)] if k != n // 2 else [(out, 0, half), (outs[n], half, groups)]
        for target, low, high in split:
            target[:, :, :rows] = own_ref[low:high, spot]
            target[:, :, rows:] = held_ref[low:high, spot].astype(BF)


def applied_shares(place, picked, own, other):
    groups, n, share, rows = own.shape
    columns = picked.shape[1]
    vm = pl.BlockSpec(memory_space=pltpu.VMEM)
    counts = [groups] * n + [groups // 2]
    counts[n // 2] = groups // 2
    return pl.pallas_call(
        apply_kernel,
        in_specs=[pl.BlockSpec(memory_space=pltpu.SMEM)] + [vm] * 3,
        out_specs=[vm] * (n + 1),
        out_shape=[jax.ShapeDtypeStruct((c, share, 2 * rows), BF) for c in counts],
        scratch_shapes=[pltpu.VMEM((groups, n, share, rows), F32)],
        compiler_params=pltpu.CompilerParams(vmem_limit_bytes=16 << 20),
        cost_estimate=pl.CostEstimate(
            flops=2 * rows * columns * other.shape[1], bytes_accessed=8 * rows * columns, transcendentals=0
        ),
        name="applied",
    )(place, picked, own, other)


def to_grid(x, step):
    n = lax.axis_size("grid")
    return lax.ppermute(x, "grid", [(i, (i + step) % n) for i in range(n)])


def summed_on_grid(shares):
    total = shares[0].astype(F32)
    opposite = {1: shares[4], -1: shares[8]}
    near = {1: shares[1], -1: shares[7]}
    second = {1: shares[2], -1: shares[6]}
    third = {1: shares[3], -1: shares[5]}
    opposite = {way: to_grid(x, 3 * way) for way, x in opposite.items()}
    third = {way: to_grid(x, 2 * way) for way, x in third.items()}
    second = {way: to_grid(x, way) for way, x in second.items()}
    sums = []
    for way in (1, -1):
        none = jnp.zeros_like(opposite[way])
        both = [opposite[way], none] if way == 1 else [none, opposite[way]]
        terms = near[way], second[way], third[way], jnp.concatenate(both)
        sums.append(to_grid(sum(t.astype(F32) for t in terms).astype(BF), way))
    return (total + sums[0].astype(F32) + sums[1].astype(F32)).astype(BF)


def body(orbitals, points, fitting, screened):
    n_grid = lax.axis_size("grid")
    n_plane = lax.axis_size(PLANE)
    grid_index = lax.axis_index("grid")
    plane_index = lax.axis_index(PLANE)
    y, xh, core, pts = (lax.axis_index(a) for a in PLANE)
    rows_dev, width = orbitals.shape
    nrows = rows_dev * n_grid
    nfull = width * lax.axis_size(ORB)
    npoints = points.shape[0]
    row_block = npoints // n_plane
    column_block = npoints // n_grid
    share = nfull // (n_plane * n_grid)
    part = rows_dev // 2
    quarter = nrows // 4

    own_rows = lax.dynamic_slice_in_dim(orbitals, pts * part, part, 0)
    held = sent_to_all(own_rows, "grid").reshape(2, quarter, width)
    alpha, beta = held[0], held[1]
    alphas = [alpha, from_next(alpha, 1), from_next(alpha, 2), from_next(alpha, -1)]
    betas = [beta, with_twin(beta), with_mirror(beta), with_far(beta)]
    a_first, a_second = jnp.stack(alphas[:2]), jnp.stack(alphas[2:])
    b_first, b_second = jnp.stack(betas[:2]), jnp.stack(betas[2:])
    pieces = [x for part in along_x(a_first, a_second) + along_y(b_first, b_second) for x in part]

    copies = jnp.broadcast_to(fitting, (n_grid, *fitting.shape))
    fit_own = lax.all_to_all(copies, "grid", 0, 0, tiled=True).reshape(nrows, row_block)
    fit_other = other_core(fit_own)

    mine = lax.dynamic_slice_in_dim(points, plane_index * row_block, row_block, 0)
    theirs_index = plane_index + (1 - 2 * core) * lax.axis_size("pts")
    theirs = lax.dynamic_slice_in_dim(points, theirs_index * row_block, row_block, 0)
    block = lax.dynamic_slice_in_dim(points, grid_index * column_block, column_block, 0)
    wanted = jnp.concatenate([mine, theirs, block])
    place = jnp.stack([pts, y, xh])
    density, density_other, picked, columns = pick(wanted, place, pieces, row_block)

    density = density + other_core(density_other)
    masked = (density * screened.astype(F32)).astype(BF)
    masked_other = other_core(masked)
    applied_own = applied_rows(picked, masked, n_grid, share)
    masked_other, fit_own = lax.optimization_barrier((masked_other, fit_own))

    applied = summed_on_grid(
        applied_shares(grid_index[None], picked, applied_own, masked_other)
    )
    applied = applied.reshape(-1, 2 * row_block)
    terms = sum(
        lax.dot_general(a, f, (((1,), (1,)), ((), ())), preferred_element_type=F32)
        for a, f in ((applied[:, :row_block], fit_own), (applied[:, row_block:], fit_other))
    ).astype(BF)
    parts = lax.all_to_all(terms.reshape(-1, share, nrows), CHIPS, 0, 0, tiled=True)
    exchange = -jnp.sum(parts.astype(F32), axis=0)
    exchange = jnp.stack([exchange, other_core(exchange)])
    exchange = jnp.where(core == 0, exchange, exchange[::-1])

    rounded = exchange.astype(BF).reshape(2 * share, nrows)
    matrix = lax.dot_general(
        rounded, columns, (((1,), (1,)), ((), ())), preferred_element_type=F32
    ) / math.sqrt(nrows)
    matrix = matrix.reshape(2, share, n_grid, width).transpose(2, 0, 1, 3)
    mine = exchange.reshape(2, share, n_grid, 2, width)
    mine = lax.dynamic_index_in_dim(mine, core, 3, keepdims=False).transpose(2, 0, 1, 3)
    both = jnp.stack([mine, matrix], axis=2).reshape(2 * n_grid, 2, share, width)
    both = lax.all_to_all(both, ("grid", "core"), 0, 0, tiled=True)
    both = both.reshape(n_grid, 2, 2, share, width).transpose(2, 0, 3, 1, 4)
    both = both.reshape(2, n_grid * share, 2 * width)
    return both[0], both[1]


def solution(mesh):
    n_grid, n_orb, n_pts = (mesh.shape[a] for a in ("grid", "orb", "pts"))
    fine = Mesh(
        mesh.devices.reshape(n_grid, n_orb // 4, 2, 2, n_pts),
        ("grid", "y", "xh", "core", "pts"),
    )
    in_specs = (P("grid", ORB), P(), P("grid", PLANE), P(PLANE, "grid"))
    out_specs = (P(PLANE, "grid"), P(PLANE, "grid"))
    return jax.shard_map(body, mesh=fine, in_specs=in_specs, out_specs=out_specs, check_vma=False)
```
